256 devices in a mesh: region: 64 (over y, z, core), strip: 4 (over x).
Axes of the slice: x: 4, y: 4, z: 8, core: 2. Of those that a mesh axis runs over, the one named last changes fastest.
Arguments:
- features: bfloat16 [32, 512, 32, 128], P(None, 'region', 'strip'), may hold values from -28 to 28
- brick_mask: int32 [64, 4, 16], P('region', 'strip'), may hold values from 0 to 1, as said below
- conv_first: bfloat16 [3, 3, 3, 32, 32], replicated, may hold values from -0.21875 to 0.21875
- conv_second: bfloat16 [3, 3, 3, 32, 32], replicated, may hold values from -0.21875 to 0.21875
- gain_first: float32 [32], replicated, may hold values from 0.5 to 1.5
- shift_first: float32 [32], replicated, may hold values from -2 to 2
- gain_second: float32 [32], replicated, may hold values from 0.5 to 1.5
- shift_second: float32 [32], replicated, may hold values from -2 to 2
Outputs:
- block_out: bfloat16 [32, 512, 32, 128], P(None, 'region', 'strip')
The draws below stay inside these ranges and needn't reach their ends.
Inputs may be any that keep to these rules, and one draw needn't show every extreme that they name: `brick_mask`: every device's block of 1 x 1 x 16 bricks holds at least one active brick.
All inputs are finite; a program needn't handle non-finite values.
Results may differ from the reference program's by a relative error of at most 0.0085.
Values may be sent and summed in bfloat16 or wider, within the bound.
A program may use at most 64 MiB of HBM per device.

```python
import math
import jax
import jax.numpy as jnp
from jax import lax

C = 32
BRICK = 8
BXD = 1
BYD = 1
BZ = 16
NZ = 128
NXB = 64
NYB = 4
NX = 512
NY = 32


def smooth_field(key):
    field = jnp.clip(jax.random.normal(key, (NX, NY, NZ), jnp.float32), -3.0, 3.0)
    for direction in range(3):
        margins = [(0, 0), (0, 0), (0, 0)]
        margins[direction] = (2, 2)
        padded = jnp.pad(field, margins)
        extent = field.shape[direction]
        running = jnp.zeros_like(field)
        for displacement in range(5):
            running = running + lax.slice_in_dim(padded, displacement, displacement + extent, axis=direction)
        field = running / math.sqrt(5.0)
    return jnp.clip(field, -3.0, 3.0)


def draw_features(key, part):
    rough = jnp.clip(jax.random.normal(jax.random.fold_in(key, 11), (C, NX, NY, NZ), jnp.float32), -3.0, 3.0)
    common = smooth_field(jax.random.fold_in(key, 12))[None]
    place_x = lax.broadcasted_iota(jnp.float32, (1, NX, 1, 1), 1) / max(NX - 1, 1)
    place_y = lax.broadcasted_iota(jnp.float32, (1, 1, NY, 1), 2) / max(NY - 1, 1)
    channel_offset = jnp.clip(jax.random.normal(jax.random.fold_in(key, 14), (C, 1, 1, 1), jnp.float32), -1.0, 1.0)
    mixing = 0.15 + 0.7 * place_x
    amplitude = (0.5 + place_x) * (0.5 + 1.5 * place_y)
    noise = jnp.sqrt(1.0 - mixing * mixing) * rough + mixing * common
    return (noise * amplitude + channel_offset * amplitude).astype(jnp.bfloat16)


def draw_brick_mask(key, part):
    place_x = lax.broadcasted_iota(jnp.int32, (NXB, NYB, BZ), 0)
    place_y = lax.broadcasted_iota(jnp.int32, (NXB, NYB, BZ), 1)
    threshold = 150 + 450 * place_x // max(NXB - 1, 1) + 300 * place_y // max(NYB - 1, 1)
    rolls = jax.random.randint(jax.random.fold_in(key, 21), (NXB, NYB, BZ), 0, 1000)
    active = (rolls < threshold).astype(jnp.int32)
    blocks_x = NXB // BXD
    blocks_y = NYB // BYD
    chosen = jax.random.randint(jax.random.fold_in(key, 22), (blocks_x, 1, blocks_y, 1, 1), 0, BXD * BYD * BZ)
    inner_x = lax.broadcasted_iota(jnp.int32, (1, BXD, 1, BYD, BZ), 1)
    inner_y = lax.broadcasted_iota(jnp.int32, (1, BXD, 1, BYD, BZ), 3)
    inner_z = lax.broadcasted_iota(jnp.int32, (1, BXD, 1, BYD, BZ), 4)
    position = (inner_x * BYD + inner_y) * BZ + inner_z
    forced = (position == chosen).astype(jnp.int32).reshape(NXB, NYB, BZ)
    return jnp.maximum(active, forced)


def bell_draw(own_key, shape, scale, most, kind=jnp.bfloat16):
    values = scale * jax.random.normal(own_key, shape, jnp.float32)
    return jnp.clip(values, min=-most, max=most).astype(kind)


def setup_inputs(seed: int = 0) -> dict:
    keys = jax.random.split(jax.random.key(seed), 9)
    return {
        "features": draw_features(jax.random.fold_in(keys[8], 71), 0),
        "brick_mask": draw_brick_mask(jax.random.fold_in(keys[8], 71), 0),
        "conv_first": bell_draw(keys[2], (3, 3, 3, C, C), (27 * C) ** -0.5, 0.21875),
        "conv_second": bell_draw(keys[3], (3, 3, 3, C, C), (27 * C) ** -0.5, 0.21875),
        "gain_first": jnp.clip(1.0 + 0.1 * jax.random.normal(keys[4], (C,), jnp.float32), 0.5, 1.5),
        "shift_first": bell_draw(keys[5], (C,), 0.5, 2.0, jnp.float32),
        "gain_second": jnp.clip(1.0 + 0.1 * jax.random.normal(keys[6], (C,), jnp.float32), 0.5, 1.5),
        "shift_second": bell_draw(keys[7], (C,), 0.5, 2.0, jnp.float32),
    }


EPSILON = 1e-05

def expand(bricks):
    count_x, count_y, count_z = bricks.shape
    values = bricks.astype(jnp.float32)
    grown = jnp.broadcast_to(values[:, None, :, None, :, None], (count_x, BRICK, count_y, BRICK, count_z, BRICK))
    return grown.reshape(count_x * BRICK, count_y * BRICK, count_z * BRICK)

def convolve_grid(field, weight, voxel_mask):
    padded = jnp.pad(field, ((0, 0), (1, 1), (1, 1), (1, 1)))
    slab_width = BRICK * BXD
    blocks_total = NX // slab_width

    def slab_conv(block_index):
        offset = (block_index * slab_width).astype(jnp.int32)
        window_in = lax.dynamic_slice_in_dim(padded, offset, slab_width + 2, 1).astype(jnp.float32)
        running = jnp.zeros((C, slab_width, NY, NZ), jnp.float32)
        for step_x in range(3):
            for step_y in range(3):
                for step_z in range(3):
                    kernel = weight[step_x, step_y, step_z].astype(jnp.float32)
                    part_in = window_in[:, step_x:step_x + slab_width, step_y:step_y + NY, step_z:step_z + NZ]
                    running = running + jnp.einsum('io,ixyz->oxyz', kernel, part_in, precision=lax.Precision.HIGHEST)
        slab_mask = lax.dynamic_slice_in_dim(voxel_mask, offset, slab_width, 0)
        return (running * slab_mask).astype(jnp.bfloat16)
    stacked = lax.map(slab_conv, jnp.arange(blocks_total, dtype=jnp.int32))
    return stacked.transpose(1, 0, 2, 3, 4).reshape(C, NX, NY, NZ)

def moments(field, voxel_mask):
    active_total = jnp.sum(voxel_mask)

    def channel_stats(plane):
        values = plane.astype(jnp.float32)
        average = jnp.sum(values * voxel_mask) / active_total
        centered = (values - average) * voxel_mask
        return (average, jnp.sum(centered * centered) / active_total)
    return lax.map(channel_stats, field)

def normalized(field, voxel_mask, gain, shift, residual):
    average, variance = moments(field, voxel_mask)
    scale = lax.rsqrt(variance + EPSILON) * gain

    def channel_out(items):
        plane, mean_c, scale_c, shift_c, extra = items
        values = (plane.astype(jnp.float32) - mean_c) * scale_c + shift_c + extra.astype(jnp.float32)
        return (jax.nn.relu(values) * voxel_mask).astype(jnp.bfloat16)
    return lax.map(channel_out, (field, average, scale, shift, residual))

def reference(features, brick_mask, conv_first, conv_second, gain_first, shift_first, gain_second, shift_second):
    voxel_mask = expand(brick_mask)
    masked_input = features * voxel_mask.astype(jnp.bfloat16)
    first_out = convolve_grid(masked_input, conv_first, voxel_mask)
    activation = normalized(first_out, voxel_mask, gain_first, shift_first, jnp.zeros_like(first_out))
    second_out = convolve_grid(activation, conv_second, voxel_mask)
    return normalized(second_out, voxel_mask, gain_second, shift_second, masked_input)
```

```python
import functools

import jax
import jax.numpy as jnp
from jax import lax
from jax.experimental import pallas as pl
from jax.experimental.pallas import tpu as pltpu
from jax.sharding import PartitionSpec as P

MESH = pl.DeviceIdType.MESH
EPSILON = 1e-05
C = 32
NX = 8
NY = 8
NZ = 128
ROWS = C * NY
TAPS = 27
HOLE = -1e30
F32 = jnp.float32
BF16 = jnp.bfloat16
NT = (((1,), (1,)), ((), ()))
SIDES = ((1, 0), (-1, 0), (0, 1), (0, -1), (1, 1), (1, -1), (-1, 1), (-1, -1))


def three_parts(value, axis):
    high = value.astype(BF16)
    rest = value - high.astype(F32)
    middle = rest.astype(BF16)
    low = (rest - middle.astype(F32)).astype(BF16)
    return jnp.concatenate([high, middle, low], axis=axis)


def iota(shape, dim):
    return lax.broadcasted_iota(jnp.int32, shape, dim)


def one_hot(condition):
    return jnp.where(condition, 1.0, 0.0).astype(BF16)


def kernel(
    regions,
    strips,
    features,
    bricks,
    conv_first,
    conv_second,
    gain_first,
    shift_first,
    gain_second,
    shift_second,
    out,
    raw,
    bricks_v,
    weights,
    affine,
    plane_f,
    input_x,
    input_y,
    side_send,
    mid_x,
    mid_y,
    mid_send,
    act_x,
    act_y,
    second,
    spread,
    pick_main,
    pick_side,
    weights_rep,
    banded,
    final,
    gathered,
    load_sem,
    param_sem,
    store_sem,
    halo_send_sem,
    halo_recv_sem,
    sum_send_sem,
    sum_recv_sem,
):
    region = lax.axis_index("region")
    strip = lax.axis_index("strip")
    near = regions // 4
    high = lax.div(region, near)
    low = lax.rem(region, near)
    wide = 4 * strips
    cross = high * strips + strip

    loads = [
        pltpu.make_async_copy(features.at[:, x], raw.at[x], load_sem.at[x]) for x in range(NX)
    ]
    params = [
        pltpu.make_async_copy(source, target, param_sem.at[j])
        for j, (source, target) in enumerate(
            (
                (bricks, bricks_v),
                (conv_first, weights.at[0, pl.ds(0, TAPS * C)]),
                (conv_second, weights.at[1, pl.ds(0, TAPS * C)]),
                (gain_first, affine.at[0]),
                (shift_first, affine.at[1]),
                (gain_second, affine.at[2]),
                (shift_second, affine.at[3]),
            )
        )
    ]
    for copy in params[:1] + loads + params[1:]:
        copy.start()

    def there(dr, ds):
        ok = jnp.bool_(True)
        if dr > 0:
            ok = jnp.logical_and(ok, region < regions - 1)
        if dr < 0:
            ok = jnp.logical_and(ok, region > 0)
        if ds > 0:
            ok = jnp.logical_and(ok, strip < strips - 1)
        if ds < 0:
            ok = jnp.logical_and(ok, strip > 0)
        return ok

    def near_peer(k):
        return {"region": high * near + lax.rem(low + k, near), "strip": strip}

    def cross_peer(k):
        q = lax.rem(cross + k, wide)
        return {"region": lax.div(q, strips) * near + low, "strip": lax.rem(q, strips)}

    for side in (0, NX + 1):
        input_x[side] = jnp.zeros((ROWS, NZ), BF16)
        mid_x[side] = jnp.full((ROWS, NZ), HOLE, BF16)
    input_y[...] = jnp.zeros(input_y.shape, BF16)
    mid_y[...] = jnp.full(mid_y.shape, HOLE, BF16)
    act_y[...] = jnp.zeros(act_y.shape, BF16)
    weights[:, TAPS * C :, :] = jnp.zeros((2, C, C), BF16)

    barrier = pltpu.get_barrier_semaphore()
    expected = jnp.int32(near - 1 + wide - 1)
    for dr, ds in SIDES:

        @pl.when(there(dr, ds))
        def _():
            pl.semaphore_signal(
                barrier,
                inc=1,
                device_id={"region": region + dr, "strip": strip + ds},
                device_id_type=MESH,
            )

        expected = expected + there(dr, ds).astype(jnp.int32)

    @pl.loop(1, near)
    def _(k):
        pl.semaphore_signal(barrier, inc=1, device_id=near_peer(k), device_id_type=MESH)

    @pl.loop(1, wide)
    def _(k):
        pl.semaphore_signal(barrier, inc=1, device_id=cross_peer(k), device_id_type=MESH)

    def halo_copies(rnd, planes, edges, sides):
        pieces = {
            (1, 0): (planes.at[NX], planes.at[0]),
            (-1, 0): (planes.at[1], planes.at[NX + 1]),
            (0, 1): (edges.at[1], sides.at[pl.ds(1, NX), pl.ds(0, C)]),
            (0, -1): (edges.at[0], sides.at[pl.ds(1, NX), pl.ds(C, C)]),
            (1, 1): (edges.at[1, NX - 1], sides.at[0, pl.ds(0, C)]),
            (1, -1): (edges.at[0, NX - 1], sides.at[0, pl.ds(C, C)]),
            (-1, 1): (edges.at[1, 0], sides.at[NX + 1, pl.ds(0, C)]),
            (-1, -1): (edges.at[0, 0], sides.at[NX + 1, pl.ds(C, C)]),
        }
        return [
            pltpu.make_async_remote_copy(
                src_ref=pieces[dr, ds][0],
                dst_ref=pieces[dr, ds][1],
                send_sem=halo_send_sem.at[rnd, j],
                recv_sem=halo_recv_sem.at[rnd, j],
                device_id={"region": region + dr, "strip": strip + ds},
                device_id_type=MESH,
            )
            for j, (dr, ds) in enumerate(SIDES)
        ]

    first_halo = halo_copies(0, input_x, side_send, input_y)
    second_halo = halo_copies(1, mid_x, mid_send, mid_y)

    def send_halo(copies):
        for copy, (dr, ds) in zip(copies, SIDES):

            @pl.when(there(dr, ds))
            def _():
                copy.start()

    def receive_halo(copies):
        for copy, (dr, ds) in zip(copies, SIDES):

            @pl.when(there(-dr, -ds))
            def _():
                copy.wait_recv()

    params[0].wait()
    brick_rows = jnp.broadcast_to(bricks_v[...].astype(F32), (8, NZ // 8)).astype(BF16)
    brick_lanes = one_hot(iota((NZ // 8, NZ), 1) // 8 == iota((NZ // 8, NZ), 0))
    mask = jnp.dot(brick_rows, brick_lanes, preferred_element_type=F32)[0:1]
    count = jnp.sum(mask, axis=1, keepdims=True) * float(NX * NY)

    @pl.loop(0, NX)
    def _(x):
        pltpu.make_async_copy(features.at[:, x], raw.at[x], load_sem.at[x]).wait()
        plane = raw[x].astype(F32).reshape(ROWS, NZ) * mask
        input_x[x + 1] = plane.astype(BF16)
        plane_f[...] = plane
        side_send[0, x] = plane_f[pl.ds(0, C, stride=NY), :].astype(BF16)
        side_send[1, x] = plane_f[pl.ds(NY - 1, C, stride=NY), :].astype(BF16)

    pl.semaphore_wait(barrier, expected)
    send_halo(first_halo)

    spread[...] = one_hot(iota((ROWS, C), 0) // NY == iota((ROWS, C), 1))
    for j in range(4):
        pick_main[j] = one_hot(iota((NZ, ROWS), 0) == j * C + iota((NZ, ROWS), 1) // NY)
    lane = iota((TAPS * C + C, ROWS), 1)
    wanted = ((lane // 64) * 9 + 6 * ((lane // C) % 2)) * C + lane % C
    wanted = jnp.where(lane < 192, wanted, -(1 << 20))
    for dz in range(3):
        pick_side[dz] = one_hot(iota((TAPS * C + C, ROWS), 0) == wanted + dz * C)

    for copy in params[1:]:
        copy.wait()

    def build(which):
        weights_rep[...] = lax.dot_general(
            spread[...], weights[which], NT, preferred_element_type=F32
        ).astype(BF16)
        row = iota((ROWS, ROWS), 0) % NY
        step = iota((ROWS, ROWS), 1) % NY - row

        @pl.loop(0, 9)
        def _(n):
            dx = lax.div(n, 3)
            dz = lax.rem(n, 3)
            total = jnp.zeros((ROWS, ROWS), F32)
            for dy in range(3):
                tap = dx * 9 + dy * 3 + dz
                block = pl.multiple_of(lax.div(tap, 4) * NZ, NZ)
                part = jnp.dot(
                    weights_rep[:, pl.ds(block, NZ)],
                    pick_main[lax.rem(tap, 4)],
                    preferred_element_type=F32,
                )
                total = jnp.where(step == dy - 1, part, total)
            banded[
                pl.ds(pl.multiple_of(dz * ROWS, ROWS), ROWS),
                pl.ds(pl.multiple_of(dx * ROWS, ROWS), ROWS),
            ] = total.astype(BF16)

        side = (iota((ROWS, ROWS), 1) // C) % 2
        kept = jnp.logical_or(
            jnp.logical_and(side == 0, row == 0), jnp.logical_and(side == 1, row == NY - 1)
        )
        for dz in range(3):
            part = jnp.dot(weights_rep[...], pick_side[dz], preferred_element_type=F32)
            banded[dz * ROWS : (dz + 1) * ROWS, 3 * ROWS :] = jnp.where(kept, part, 0.0).astype(
                BF16
            )

    def plane_pair(planes, sides, x):
        def column(at):
            return jnp.concatenate(
                [
                    planes[pl.ds(at, 3)].reshape(3 * ROWS, NZ),
                    sides[pl.ds(at, 4)].reshape(ROWS, NZ),
                ],
                axis=0,
            )

        both = jnp.concatenate([column(x), column(x + 1)], axis=1)
        raw_out = jnp.dot(banded[...], both, preferred_element_type=F32)
        lanes = iota((ROWS, NZ), 1)
        results = []
        for p in range(2):
            below, here, above = (
                raw_out[dz * ROWS : (dz + 1) * ROWS, p * NZ : (p + 1) * NZ] for dz in range(3)
            )
            below = jnp.where(lanes == 0, 0.0, pltpu.roll(below, 1, 1))
            above = jnp.where(lanes == NZ - 1, 0.0, pltpu.roll(above, NZ - 1, 1))
            summed = (here + below + above) * mask
            results.append(summed.astype(BF16).astype(F32))
        return results

    def row_of_sums(sums, squares):
        folded = jnp.dot(
            jnp.concatenate([fold] * 3, axis=1),
            three_parts(jnp.concatenate([sums, squares], axis=1), 0),
            preferred_element_type=F32,
        )
        stacked = jnp.concatenate(
            [folded[:, :NZ], folded[:, NZ:], jnp.zeros((2 * C, NZ), F32)], axis=0
        )
        totals = lax.dot_general(
            jnp.ones((8, 3 * NZ), BF16), three_parts(stacked, 1), NT, preferred_element_type=F32
        )[0:1]
        return jnp.where(iota((1, NZ), 1) == 2 * C, count, totals)

    def sum_copy(rnd, phase, slot, k, peer):
        return pltpu.make_async_remote_copy(
            src_ref=gathered.at[rnd, phase, slot],
            dst_ref=gathered.at[rnd, phase, slot],
            send_sem=sum_send_sem.at[rnd, phase, k],
            recv_sem=sum_recv_sem.at[rnd, phase, slot],
            device_id=peer,
            device_id_type=MESH,
        )

    def phase_send(rnd, phase, size, slot, peers, value):
        gathered[rnd, phase, slot] = value

        @pl.loop(1, size)
        def _(k):
            sum_copy(rnd, phase, slot, k, peers(k)).start()

    def phase_receive(rnd, phase, size, slot, peers):
        @pl.loop(1, size)
        def _(k):
            sum_copy(rnd, phase, lax.rem(slot + k, size), k, peers(k)).wait_recv()

        total = gathered[rnd, phase, 0]
        for k in range(1, size):
            total = total + gathered[rnd, phase, k]
        return total

    def phase_finish(rnd, phase, size, slot, peers):
        @pl.loop(1, size)
        def _(k):
            sum_copy(rnd, phase, slot, k, peers(k)).wait_send()

    expand = jnp.concatenate(
        [
            one_hot(iota((ROWS, C), 0) // NY == iota((ROWS, C), 1)),
            one_hot(iota((2 * C, C), 0) % C == iota((2 * C, C), 1)),
        ],
        axis=0,
    )
    fold = one_hot(iota((C, ROWS), 1) // NY == iota((C, ROWS), 0))

    def columns(total, gain, shift):
        active = total[:, 2 * C : 2 * C + 1]
        average = total[:, :C] / active
        variance = total[:, C : 2 * C] / active - average * average
        scale = lax.rsqrt(variance + EPSILON) * gain
        offset = shift - average * scale
        rows = jnp.concatenate(
            [jnp.broadcast_to(scale, (NZ, C)), jnp.broadcast_to(offset, (NZ, C))], axis=0
        )
        both = lax.dot_general(
            jnp.concatenate([expand] * 3, axis=1),
            three_parts(rows, 1),
            NT,
            preferred_element_type=F32,
        )
        return both[:, :NZ], both[:, NZ:]

    build(0)
    receive_halo(first_halo)

    sums = jnp.zeros((ROWS, NZ), F32)
    squares = jnp.zeros((ROWS, NZ), F32)
    for x in range(0, NX, 2):
        for p, value in enumerate(plane_pair(input_x, input_y, x)):
            sums = sums + value
            squares = squares + value * value
            held = jnp.where(mask > 0.0, value, HOLE)
            mid_x[x + p + 1] = held.astype(BF16)
            plane_f[...] = held
            mid_send[0, x + p] = plane_f[pl.ds(0, C, stride=NY), :].astype(BF16)
            mid_send[1, x + p] = plane_f[pl.ds(NY - 1, C, stride=NY), :].astype(BF16)

    phase_send(0, 0, near, low, near_peer, row_of_sums(sums, squares))
    send_halo(second_halo)
    build(1)
    partial = phase_receive(0, 0, near, low, near_peer)
    phase_send(0, 1, wide, cross, cross_peer, partial)
    receive_halo(second_halo)
    total = phase_receive(0, 1, wide, cross, cross_peer)

    scale, offset = columns(total, affine[0], affine[1])
    for x in range(NX + 2):
        value = mid_x[x].astype(F32) * scale[:ROWS] + offset[:ROWS]
        act_x[x] = jnp.maximum(value, 0.0).astype(BF16)
        value = mid_y[x].astype(F32) * scale[ROWS:] + offset[ROWS:]
        act_y[x] = jnp.maximum(value, 0.0).astype(BF16)

    sums = jnp.zeros((ROWS, NZ), F32)
    squares = jnp.zeros((ROWS, NZ), F32)
    for x in range(0, NX, 2):
        for p, value in enumerate(plane_pair(act_x, act_y, x)):
            sums = sums + value
            squares = squares + value * value
            second[x + p] = value.astype(BF16)

    phase_send(1, 0, near, low, near_peer, row_of_sums(sums, squares))
    partial = phase_receive(1, 0, near, low, near_peer)
    phase_send(1, 1, wide, cross, cross_peer, partial)
    total = phase_receive(1, 1, wide, cross, cross_peer)

    scale, offset = columns(total, affine[2], affine[3])
    for x in range(NX):
        value = second[x].astype(F32) * scale[:ROWS] + offset[:ROWS]
        value = jnp.maximum(value + input_x[x + 1].astype(F32), 0.0) * mask
        final[x] = value.reshape(C, NY, NZ).astype(BF16)
        pltpu.make_async_copy(final.at[x], out.at[:, x], store_sem.at[x]).start()

    for copies in (first_halo, second_halo):
        for copy, (dr, ds) in zip(copies, SIDES):

            @pl.when(there(dr, ds))
            def _():
                copy.wait_send()

    for rnd in range(2):
        phase_finish(rnd, 0, near, low, near_peer)
        phase_finish(rnd, 1, wide, cross, cross_peer)
    for x in range(NX):
        pltpu.make_async_copy(final.at[x], out.at[:, x], store_sem.at[x]).wait()


def solution(mesh):
    regions, strips = mesh.shape["region"], mesh.shape["strip"]
    most = max(regions // 4, 4 * strips)

    def per_device(features, bricks, conv_first, conv_second, *affine):
        rows = (TAPS * C, C)
        return pl.pallas_call(
            functools.partial(kernel, regions, strips),
            out_shape=jax.ShapeDtypeStruct(features.shape, BF16),
            in_specs=[pl.BlockSpec(memory_space=pl.ANY)] * 8,
            out_specs=pl.BlockSpec(memory_space=pl.ANY),
            scratch_shapes=[
                pltpu.VMEM((NX, C, NY, NZ), BF16),
                pltpu.VMEM((1, NZ // 8), jnp.int32),
                pltpu.VMEM((2, TAPS * C + C, C), BF16),
                pltpu.VMEM((4, 1, C), F32),
                pltpu.VMEM((ROWS, NZ), F32),
                pltpu.VMEM((NX + 2, ROWS, NZ), BF16),
                pltpu.VMEM((NX + 4, 2 * C, NZ), BF16),
                pltpu.VMEM((2, NX, C, NZ), BF16),
                pltpu.VMEM((NX + 2, ROWS, NZ), BF16),
                pltpu.VMEM((NX + 2, 2 * C, NZ), BF16),
                pltpu.VMEM((2, NX, C, NZ), BF16),
                pltpu.VMEM((NX + 2, ROWS, NZ), BF16),
                pltpu.VMEM((NX + 4, 2 * C, NZ), BF16),
                pltpu.VMEM((NX, ROWS, NZ), BF16),
                pltpu.VMEM((ROWS, C), BF16),
                pltpu.VMEM((4, NZ, ROWS), BF16),
                pltpu.VMEM((3, TAPS * C + C, ROWS), BF16),
                pltpu.VMEM((ROWS, TAPS * C + C), BF16),
                pltpu.VMEM((3 * ROWS, 4 * ROWS), BF16),
                pltpu.VMEM((NX, C, NY, NZ), BF16),
                pltpu.VMEM((2, 2, most, 1, NZ), F32),
                pltpu.SemaphoreType.DMA((NX,)),
                pltpu.SemaphoreType.DMA((7,)),
                pltpu.SemaphoreType.DMA((NX,)),
                pltpu.SemaphoreType.DMA((2, 8)),
                pltpu.SemaphoreType.DMA((2, 8)),
                pltpu.SemaphoreType.DMA((2, 2, most)),
                pltpu.SemaphoreType.DMA((2, 2, most)),
            ],
            compiler_params=pltpu.CompilerParams(
                collective_id=0, has_side_effects=True, vmem_limit_bytes=48 * 1024 * 1024
            ),
            name="block",
        )(
            features,
            bricks.reshape(1, NZ // 8),
            conv_first.reshape(rows),
            conv_second.reshape(rows),
            *(a.reshape(1, C) for a in affine),
        )

    placed = P(None, "region", "strip", None)
    return jax.shard_map(
        per_device,
        mesh=mesh,
        in_specs=(placed, P("region", "strip", None)) + (P(),) * 6,
        out_specs=placed,
        check_vma=False,
    )
```
